512 devices in a mesh: blk: 32 (over y, z_hi, core), col: 16 (over x, z_lo).
Axes of the slice: x: 4, y: 8, z: 8 (z_hi: 2, z_lo: 4; z = z_hi * 4 + z_lo), core: 2. Of those that a mesh axis runs over, the one named last changes fastest.
Arguments:
- queries: bfloat16 [16384, 2048], P('blk', 'col'), may hold values from -1200 to 1200
- keys: bfloat16 [16384, 512], P(('blk', 'col')), may hold values from -4 to 4
- values: bfloat16 [16384, 512], P(('blk', 'col')), may hold values from -6 to 6
- positions: int32 [16384], P('blk'), may hold values from 0 to 16383, as said below
Outputs:
- attended: float32 [16384, 2048], P('blk', 'col')
- log_norm: float32 [16384, 16], P('blk', 'col')
The draws below stay inside these ranges and needn't reach their ends.
Inputs may be any that keep to these rules, and one draw needn't show every extreme that they name: A permutation of 0 to 16383 made of runs of 128 consecutive positions, each run stored ascending in 128 consecutive rows that start at a multiple of 128.
All inputs are finite; a program needn't handle non-finite values.
Results may differ from the reference program's by a relative error of at most 0.0034.
Values may be sent and summed in bfloat16 or wider, within the bound.
No kernel may reach another device: no remote copies, remote signals or barrier semaphores. Data moves between devices by JAX's collectives and lax.ppermute only.
A program may use at most 64 MiB of HBM per device.

```python
import math
import jax
import jax.numpy as jnp
from jax import lax

HQ = 16
HK = 4
DH = 128
STRIPE = 128
SEQ = 16384


def joint_draw(key):
    base_keys = jnp.clip(jax.random.normal(jax.random.fold_in(key, 11), (SEQ, HK, DH), jnp.float32), -4.0, 4.0)
    base_queries = jnp.clip(2.0 * jax.random.normal(jax.random.fold_in(key, 13), (SEQ, HQ, DH), jnp.float32), -8.0, 8.0)
    return (base_queries.reshape(SEQ, HQ * DH), base_keys.reshape(SEQ, HK * DH))


def draw_queries(key, part):
    return joint_draw(key)[0].astype(jnp.bfloat16)


def draw_keys(key, part):
    return joint_draw(key)[1].astype(jnp.bfloat16)


def draw_positions(key, part):
    order = jax.random.permutation(jax.random.fold_in(key, 5), SEQ // STRIPE)
    spread = order[:, None] * STRIPE + jnp.arange(STRIPE)[None, :]
    return spread.reshape(SEQ).astype(jnp.int32)


def block_scale(rng, extent, pieces, low, largest):
    gain = 1.0
    for position, blocks in pieces:
        steps = jax.random.uniform(jax.random.fold_in(jax.random.fold_in(rng, 6), position), (blocks,), jnp.float32, low / len(pieces), largest / len(pieces))
        gain = gain * jnp.repeat(jnp.exp(steps), extent[position] // blocks).reshape((-1,) + (1,) * (len(extent) - 1 - position))
    return gain


def scatter_about(rng, dims, deviation, reach, cuts=(), kind=jnp.bfloat16):
    values = deviation * jax.random.normal(rng, dims, jnp.float32)
    if cuts:
        values = values * block_scale(rng, dims, cuts, -0.22, 0.18)
    return jnp.clip(values, -reach, reach).astype(kind)


def setup_inputs(seed: int = 0) -> dict:
    arg_keys = jax.random.split(jax.random.key(seed), 5)
    return {
        "queries": draw_queries(jax.random.fold_in(arg_keys[4], 71), 0),
        "keys": draw_keys(jax.random.fold_in(arg_keys[4], 71), 0),
        "values": scatter_about(arg_keys[2], (SEQ, HK * DH), 1.0, 6.0, ((0, 512),)),
        "positions": draw_positions(jax.random.fold_in(arg_keys[4], 71), 0),
    }


def reference(queries, keys, values, positions):
    group = HQ // HK
    scale = 1.0 / math.sqrt(DH)
    qblock = math.gcd(SEQ, 512)
    key_heads = keys.astype(jnp.float32).reshape(SEQ, HK, DH)
    value_heads = values.astype(jnp.float32).reshape(SEQ, HK, DH)

    def one_block(inputs):
        query_rows, query_pos = inputs
        grouped = query_rows.astype(jnp.float32).reshape(qblock, HK, group, DH)
        scores = jnp.einsum('rhgd,khd->hgrk', grouped, key_heads) * scale
        visible = positions[None, :] <= query_pos[:, None]
        masked = jnp.where(visible, scores, -1e+30)
        top = lax.optimization_barrier(jnp.max(masked, axis=-1))
        weights = jnp.where(visible, jnp.exp(scores - top[..., None]), 0.0)
        total = lax.optimization_barrier(jnp.sum(weights, axis=-1))
        rounded = lax.optimization_barrier(weights.astype(jnp.bfloat16))
        summed = jnp.einsum('hgrk,khd->hgrd', rounded.astype(jnp.float32), value_heads)
        output = summed / total[..., None]
        output = output.transpose(2, 0, 1, 3).reshape(qblock, HQ * DH)
        lognorm = (top + jnp.log(total)).reshape(HQ, qblock).T
        return (output, lognorm)
    query_blocks = queries.reshape(SEQ // qblock, qblock, HQ * DH)
    pos_blocks = positions.reshape(SEQ // qblock, qblock)
    outputs, lognorms = lax.map(one_block, (query_blocks, pos_blocks))
    return (outputs.reshape(SEQ, HQ * DH), lognorms.reshape(SEQ, HQ))
```

```python
import math

import jax
import jax.numpy as jnp
from jax import lax
from jax.experimental import pallas as pl
from jax.experimental.pallas import tpu as pltpu
from jax.sharding import PartitionSpec as P

HQ = 16
HK = 4
DH = 128
STRIPE = 128
NY, NZH, NC, NX, NZL = 8, 2, 2, 4, 4
SUB = 64
NST = 8
BK = NST * SUB
ROWS = 2 * BK + 16
NQ = 8
C2 = math.log2(math.e) / math.sqrt(DH)
LN2 = math.log(2.0)
MASKED = -1e30
EMPTY = -1e29
VM = pltpu.VMEM
SM = pltpu.SMEM


def flat_groups(key):
    found = {}
    for b in range(NY * NZH * NC):
        for c in range(NX * NZL):
            k = key(b // 4, (b // 2) % 2, b % 2, c // 4, c % 4)
            found.setdefault(k, []).append(b * NX * NZL + c)
    return list(found.values())


KV_GROUPS = flat_groups(lambda y, zh, c, x, zl: (y, c, zl % 2))
OUT_GROUPS = flat_groups(lambda y, zh, c, x, zl: (y, zh, x, zl // 2))


def pairs(move):
    out = []
    for b in range(NY * NZH * NC):
        for c in range(NX * NZL):
            y, zh, co, x, zl = move(b // 4, (b // 2) % 2, b % 2, c // 4, c % 4)
            out.append((b * 16 + c, ((y % NY) * 4 + zh * 2 + co) * 16 + x * 4 + zl))
    return out


UP = pairs(lambda y, zh, c, x, zl: (y + 1, zh, c, x, zl))
DOWN = pairs(lambda y, zh, c, x, zl: (y - 1, zh, c, x, zl))
LAST = pairs(lambda y, zh, c, x, zl: (y + 1 - 2 * c, zh, c, x, zl))
CORE = pairs(lambda y, zh, c, x, zl: (y, zh, 1 - c, x, zl))
ZPAIR = pairs(lambda y, zh, c, x, zl: (y, zh, c, x, zl ^ 1))
DIAG = pairs(lambda y, zh, c, x, zl: (y, zh, 1 - c, x, zl ^ 1))


def send(value, perm):
    return lax.ppermute(value, ("blk", "col"), perm)


def call(kernel, out, in_spaces, scratch=(), alias=None, name=None, flops=0):
    vm = pl.BlockSpec(memory_space=VM)
    sm = pl.BlockSpec(memory_space=SM)
    return pl.pallas_call(
        kernel,
        out_shape=out,
        in_specs=[sm if s == "s" else vm for s in in_spaces],
        out_specs=jax.tree.map(lambda _: vm, out),
        scratch_shapes=list(scratch),
        input_output_aliases=alias or {},
        name=name,
        cost_estimate=pl.CostEstimate(flops=flops, transcendentals=0, bytes_accessed=0) if flops else None,
        compiler_params=pltpu.CompilerParams(vmem_limit_bytes=40 * 1024 * 1024),
    )


def pack_kernel(pos_ref, k_ref, v_ref, o_ref):
    tile = jnp.full((16, DH), pos_ref[0].astype(jnp.float32), jnp.float32).astype(jnp.bfloat16)
    for m in range(16):
        x = (m // 2) % 4
        o_ref[m, 0:32, :] = k_ref[:, x * DH : (x + 1) * DH]
        o_ref[m, 32:64, :] = v_ref[:, x * DH : (x + 1) * DH]
        o_ref[m, 64:80, :] = tile


def scalar_of(row):
    return jnp.max(row.astype(jnp.float32)).astype(jnp.int32)


def prep_kernel(r_ref, o_ref, v_scr, p_scr):
    pos = []
    for j in range(NST):
        m = (j // 4) * 8 + (j % 4) * 2
        pos.append(scalar_of(r_ref[m, 64:65, :]))
    for j in range(NST):
        rank = jnp.int32(0)
        for i in range(NST):
            if i != j:
                rank = rank + (pos[i] < pos[j]).astype(jnp.int32)
        p_scr[rank] = pos[j]
        m = (j // 4) * 8 + (j % 4) * 2
        at = pl.multiple_of(rank * SUB, SUB)
        kk = jnp.concatenate([r_ref[m, 0:32, :], r_ref[m + 1, 0:32, :]], axis=0)
        vv = jnp.concatenate([r_ref[m, 32:64, :], r_ref[m + 1, 32:64, :]], axis=0)
        o_ref[pl.ds(at, SUB), :] = kk
        v_scr[pl.ds(at, SUB), :] = vv.astype(jnp.float32)
    for t in range(BK // DH):
        o_ref[BK + t * DH : BK + (t + 1) * DH, :] = v_scr[t * DH : (t + 1) * DH, :].T.astype(jnp.bfloat16)
    row = lax.broadcasted_iota(jnp.int32, (16, DH), 0)
    tile = jnp.zeros((16, DH), jnp.float32)
    for r in range(NST):
        tile = jnp.where(row == r, p_scr[r].astype(jnp.float32), tile)
    o_ref[2 * BK : ROWS, :] = tile.astype(jnp.bfloat16)


def qext_kernel(pos_ref, q_ref, o_ref):
    o_ref[0:512, :] = q_ref[...]
    row = lax.broadcasted_iota(jnp.int32, (16, DH), 0)
    tile = jnp.zeros((16, DH), jnp.float32)
    for r in range(4):
        tile = jnp.where(row == r, pos_ref[r].astype(jnp.float32), tile)
    o_ref[512:528, :] = tile.astype(jnp.bfloat16)


def attend_kernel(nblocks, first, side_ref, qo_ref, qz_ref, qc_ref, qd_ref, *rest):
    blocks = rest[:nblocks]
    if first:
        acc_ref, m_ref, q_ref, off_ref, qp, qt, kp = rest[nblocks:]
        accin_ref = min_ref = None
    else:
        accin_ref, min_ref, acc_ref, m_ref, q_ref, off_ref, qp, qt, kp = rest[nblocks:]
    side = side_ref[0]
    pos = []
    for t in range(4):
        q_ref[t, 0:128, :] = qo_ref[t * 128 : (t + 1) * 128, :]
        q_ref[t, 128:256, :] = qz_ref[t * 128 : (t + 1) * 128, :]
        q_ref[4 + t, 0:128, :] = qc_ref[t * 128 : (t + 1) * 128, :]
        q_ref[4 + t, 128:256, :] = qd_ref[t * 128 : (t + 1) * 128, :]
    for ref in (qo_ref, qc_ref):
        for t in range(4):
            pos.append(scalar_of(ref[512 + t : 513 + t, :]))
    for j in range(NQ):
        rank = jnp.int32(0)
        for i in range(NQ):
            if i != j:
                rank = rank + (pos[i] < pos[j]).astype(jnp.int32)
        qp[rank] = pos[j]
        qt[rank] = jnp.int32(j)
    for n, blk in enumerate(blocks):
        for j in range(NST):
            kp[n * NST + j] = scalar_of(blk[2 * BK + j : 2 * BK + j + 1, :])
    r = lax.broadcasted_iota(jnp.int32, (SUB, 256), 0)
    lane = lax.broadcasted_iota(jnp.int32, (SUB, 256), 1)
    off_ref[...] = (r // 32) * 64 + side * 32 + r % 32 - lane % 128
    ones = jnp.ones((16, BK), jnp.bfloat16)
    if first:
        acc_ref[...] = jnp.zeros_like(acc_ref)
        m_ref[...] = jnp.full(m_ref.shape, EMPTY, jnp.float32)
    else:
        acc_ref[...] = accin_ref[...]
        m_ref[...] = min_ref[...]

    def local(qpos, t, keys):
        scores = []
        for n, blk in enumerate(blocks):
            s = lax.dot_general(
                blk[0:keys, :], q_ref[t], (((1,), (1,)), ((), ())), preferred_element_type=jnp.float32
            )
            parts = []
            for j in range(keys // SUB):
                gap = (qpos - kp[n * NST + j]) * STRIPE
                parts.append(jnp.where(off_ref[...] <= gap, s[j * SUB : (j + 1) * SUB, :] * C2, MASKED))
            scores.append(jnp.concatenate(parts, axis=0))
        top = jnp.max(scores[0], axis=0, keepdims=True)
        for s in scores[1:]:
            top = jnp.maximum(top, jnp.max(s, axis=0, keepdims=True))
        mixed = None
        for s, blk in zip(scores, blocks):
            p = jnp.exp2(s - top).astype(jnp.bfloat16)
            vt = jnp.concatenate(
                [blk[BK + i * DH : BK + (i + 1) * DH, :] for i in range(keys // DH)], axis=1
            )
            vt = jnp.concatenate([vt, ones[:, 0:keys]], axis=0)
            part = jnp.dot(vt, p, preferred_element_type=jnp.float32)
            mixed = part if mixed is None else mixed + part
        return top, mixed

    def two(i, keys):
        found = [(qt[2 * i + k],) + local(qp[2 * i + k], qt[2 * i + k], keys) for k in range(2)]
        for t, top, mixed in found:
            old = m_ref[t, 0:1, :]
            new = jnp.maximum(old, top)
            acc_ref[t] = acc_ref[t] * jnp.exp2(old - new) + mixed * jnp.exp2(top - new)
            m_ref[t] = jnp.broadcast_to(new, (8, 256))

    def pair(i, carry):
        far = qp[2 * i + 1]
        wide = kp[NST // 2] <= far
        seen = kp[0] <= far
        for n in range(1, nblocks):
            wide = jnp.logical_or(wide, kp[n * NST + NST // 2] <= far)
            seen = jnp.logical_or(seen, kp[n * NST] <= far)

        @pl.when(wide)
        def _():
            two(i, BK)

        @pl.when(jnp.logical_and(seen, jnp.logical_not(wide)))
        def _():
            two(i, BK // 2)

        return carry

    lax.fori_loop(0, NQ // 2, pair, 0)


def partial_kernel(who_ref, acc_ref, m_ref, o_ref):
    core, side = who_ref[0], who_ref[1]
    for dc in range(2):
        for dz in range(2):
            member = (core + dc - 2 * core * dc) * 2 + (side + dz - 2 * side * dz)
            rows = []
            for t in range(4):
                st = dc * 4 + t
                lanes = slice(dz * 128, dz * 128 + 128)
                total = acc_ref[st, 128:129, lanes]
                top = m_ref[st, 0:1, lanes]
                seen = total > 0.0
                inv = jnp.where(seen, 1.0 / jnp.where(seen, total, 1.0), 0.0)
                o_ref[member, t * 128 : (t + 1) * 128, :] = (acc_ref[st, 0:128, lanes] * inv).T.astype(jnp.bfloat16)
                rows.append(jnp.where(seen, top + jnp.log2(jnp.where(seen, total, 1.0)), EMPTY))
            lse = jnp.concatenate(rows, axis=0)
            hi = lse.astype(jnp.bfloat16).astype(jnp.float32)
            mid = (lse - hi).astype(jnp.bfloat16).astype(jnp.float32)
            low = lse - hi - mid
            o_ref[member, 512:528, :] = jnp.concatenate(
                [hi, mid, low, jnp.zeros((4, 128), jnp.float32)], axis=0
            ).astype(jnp.bfloat16)


def merge_kernel(i_ref, o_ref, l_ref):
    lses = []
    for m in range(4):
        tile = i_ref[m, 512:528, :].astype(jnp.float32)
        lses.append(tile[0:4] + tile[4:8] + tile[8:12])
    top = jnp.maximum(jnp.maximum(lses[0], lses[1]), jnp.maximum(lses[2], lses[3]))
    ws = [jnp.exp2(x - top) for x in lses]
    total = ws[0] + ws[1] + ws[2] + ws[3]
    l_ref[...] = (top + jnp.log2(total)) * LN2
    inv = 1.0 / total
    for t in range(4):
        out = None
        for m in range(4):
            w = jnp.broadcast_to((ws[m] * inv)[t : t + 1, :], (128, 128)).T
            part = i_ref[m, t * 128 : (t + 1) * 128, :].astype(jnp.float32) * w
            out = part if out is None else out + part
        o_ref[t * 128 : (t + 1) * 128, :] = out


def body(queries, keys, values, positions):
    bf, f32 = jnp.bfloat16, jnp.float32
    blk, col = lax.axis_index("blk"), lax.axis_index("col")
    core, side, x = blk % 2, col % 2, col // 4
    stripes = positions.reshape(4, STRIPE)[:, 0] // STRIPE
    mine = lax.dynamic_slice_in_dim(stripes, x, 1)
    who = jnp.stack([core, side]).astype(jnp.int32)
    side_arr = side.reshape(1).astype(jnp.int32)

    packed = call(pack_kernel, jax.ShapeDtypeStruct((16, 80, DH), bf), "svv", name="pack")(mine, keys, values)
    got = lax.all_to_all(packed, ("blk", "col"), 0, 0, axis_index_groups=KV_GROUPS, tiled=False)
    own = call(
        prep_kernel,
        jax.ShapeDtypeStruct((ROWS, DH), bf),
        "v",
        scratch=[VM((BK, DH), f32), SM((NST,), jnp.int32)],
        name="prep",
    )(got)
    qo = call(qext_kernel, jax.ShapeDtypeStruct((528, DH), bf), "sv", name="qext")(stripes, queries)

    up, down = [send(own, UP)], [send(own, DOWN)]
    qc, qz, qd = send(qo, CORE), send(qo, ZPAIR), send(qo, DIAG)
    qs = (side_arr, qo, qz, qc, qd)
    for step in range(2):
        up.append(send(up[-1], UP))
        down.append(send(down[-1], DOWN))
    last = send(jnp.where(core == 0, up[2], down[2]), LAST)

    state = (jax.ShapeDtypeStruct((NQ, 144, 256), f32), jax.ShapeDtypeStruct((NQ, 8, 256), f32))

    def attend(blocks, carry):
        n = len(blocks)
        first = carry is None
        kernel = lambda *refs: attend_kernel(n, first, *refs)
        scratch = [
            VM((NQ, 256, DH), bf),
            VM((SUB, 256), jnp.int32),
            SM((NQ,), jnp.int32),
            SM((NQ,), jnp.int32),
            SM((2 * NST,), jnp.int32),
        ]
        args = qs + tuple(blocks) + (() if first else carry)
        return call(
            kernel,
            state,
            "svvvv" + "v" * (n + (0 if first else 2)),
            scratch=scratch,
            alias=None if first else {5 + n: 0, 6 + n: 1},
            flops=n * 2_000_000_000,
            name=f"attend{n}",
        )(*args)

    carry = attend([own], None)
    for a, b in zip(up, down):
        carry = attend([a, b], carry)
    carry = attend([last], carry)
    part = call(partial_kernel, jax.ShapeDtypeStruct((4, 528, DH), bf), "svv", name="partial")(who, *carry)
    parts = lax.all_to_all(part, ("blk", "col"), 0, 0, axis_index_groups=OUT_GROUPS, tiled=False)
    attended, lognorm = call(
        merge_kernel,
        (jax.ShapeDtypeStruct((512, DH), f32), jax.ShapeDtypeStruct((4, 128), f32)),
        "v",
        name="merge",
    )(parts)
    return attended, lognorm.reshape(512, 1)


def solution(mesh):
    placed = (P("blk", "col"), P(("blk", "col"), None), P(("blk", "col"), None), P("blk"))
    return jax.shard_map(
        body,
        mesh=mesh,
        in_specs=placed,
        out_specs=(P("blk", "col"), P("blk", "col")),
        check_vma=False,
    )
```

```python
import math

import jax
import jax.numpy as jnp
from jax import lax
from jax.experimental import pallas as pl
from jax.experimental.pallas import tpu as pltpu
from jax.sharding import PartitionSpec as P

HQ = 16
HK = 4
DH = 128
STRIPE = 128
NY, NZH, NC, NX, NZL = 8, 2, 2, 4, 4
SUB = 64
NST = 8
BK = NST * SUB
ROWS = 2 * BK + 16
NQ = 8
C2 = math.log2(math.e) / math.sqrt(DH)
LN2 = math.log(2.0)
MASKED = -1e30
EMPTY = -1e29
VM = pltpu.VMEM
SM = pltpu.SMEM


def flat_groups(key):
    found = {}
    for b in range(NY * NZH * NC):
        for c in range(NX * NZL):
            k = key(b // 4, (b // 2) % 2, b % 2, c // 4, c % 4)
            found.setdefault(k, []).append(b * NX * NZL + c)
    return list(found.values())


KV_GROUPS = flat_groups(lambda y, zh, c, x, zl: (y, c, zl % 2))
OUT_GROUPS = flat_groups(lambda y, zh, c, x, zl: (y, zh, x, zl // 2))


def pairs(move):
    out = []
    for b in range(NY * NZH * NC):
        for c in range(NX * NZL):
            y, zh, co, x, zl = move(b // 4, (b // 2) % 2, b % 2, c // 4, c % 4)
            out.append((b * 16 + c, ((y % NY) * 4 + zh * 2 + co) * 16 + x * 4 + zl))
    return out


UP = pairs(lambda y, zh, c, x, zl: (y + 1, zh, c, x, zl))
DOWN = pairs(lambda y, zh, c, x, zl: (y - 1, zh, c, x, zl))
LAST = pairs(lambda y, zh, c, x, zl: (y + 2 - 4 * c, zh, c, x, zl))
CORE = pairs(lambda y, zh, c, x, zl: (y, zh, 1 - c, x, zl))
ZPAIR = pairs(lambda y, zh, c, x, zl: (y, zh, c, x, zl ^ 1))


def send(value, perm):
    return lax.ppermute(value, ("blk", "col"), perm)


def call(kernel, out, in_spaces, scratch=(), alias=None, name=None, flops=0):
    vm = pl.BlockSpec(memory_space=VM)
    sm = pl.BlockSpec(memory_space=SM)
    return pl.pallas_call(
        kernel,
        out_shape=out,
        in_specs=[{"s": sm, "v": vm, "h": pl.BlockSpec(memory_space=pltpu.HBM)}[s] for s in in_spaces],
        out_specs=jax.tree.map(lambda _: vm, out),
        scratch_shapes=list(scratch),
        input_output_aliases=alias or {},
        name=name,
        cost_estimate=pl.CostEstimate(flops=flops, transcendentals=0, bytes_accessed=0) if flops else None,
        compiler_params=pltpu.CompilerParams(vmem_limit_bytes=40 * 1024 * 1024),
    )


def pack_kernel(pos_hbm, k_hbm, v_hbm, q_hbm, o_ref, q_ref, pos, k_ref, v_ref, sems):
    copies = [
        pltpu.make_async_copy(src, dst, sems.at[i])
        for i, (src, dst) in enumerate(
            [(pos_hbm, pos), (k_hbm, k_ref), (v_hbm, v_ref), (q_hbm, q_ref.at[pl.ds(0, 512)])]
        )
    ]
    for c in copies:
        c.start()
    copies[0].wait()
    x = lax.axis_index("col") // NZL
    mine = pos[pl.multiple_of(x * STRIPE, STRIPE)] // STRIPE
    tile = jnp.full((8, DH), mine.astype(jnp.float32), jnp.float32).astype(jnp.bfloat16)
    for m in range(16):
        o_ref[m, 64:72, :] = tile
    row = lax.broadcasted_iota(jnp.int32, (16, DH), 0)
    tile = jnp.zeros((16, DH), jnp.float32)
    for r in range(4):
        tile = jnp.where(row == r, (pos[r * STRIPE] // STRIPE).astype(jnp.float32), tile)
    q_ref[512:528, :] = tile.astype(jnp.bfloat16)
    for at, ref, c in ((0, k_ref, copies[1]), (32, v_ref, copies[2])):
        c.wait()
        for m in range(16):
            head = (m // 2) % 4
            o_ref[m, at : at + 32, :] = ref[:, head * DH : (head + 1) * DH]
    copies[3].wait()


def scalar_of(row):
    return jnp.max(row.astype(jnp.float32)).astype(jnp.int32)


def prep_kernel(r_ref, o_ref, v_scr, p_scr):
    pos = []
    for j in range(NST):
        m = (j // 4) * 8 + (j % 4) * 2
        pos.append(scalar_of(r_ref[m, 64:65, :]))
    for j in range(NST):
        rank = jnp.int32(0)
        for i in range(NST):
            if i != j:
                rank = rank + (pos[i] < pos[j]).astype(jnp.int32)
        p_scr[rank] = pos[j]
        m = (j // 4) * 8 + (j % 4) * 2
        at = pl.multiple_of(rank * SUB, SUB)
        kk = jnp.concatenate([r_ref[m, 0:32, :], r_ref[m + 1, 0:32, :]], axis=0)
        vv = jnp.concatenate([r_ref[m, 32:64, :], r_ref[m + 1, 32:64, :]], axis=0)
        o_ref[pl.ds(at, SUB), :] = kk
        v_scr[pl.ds(at, SUB), :] = vv.astype(jnp.float32)
    for t in range(BK // DH):
        o_ref[BK + t * DH : BK + (t + 1) * DH, :] = v_scr[t * DH : (t + 1) * DH, :].T.astype(jnp.bfloat16)
    row = lax.broadcasted_iota(jnp.int32, (16, DH), 0)
    tile = jnp.zeros((16, DH), jnp.float32)
    for r in range(NST):
        tile = jnp.where(row == r, p_scr[r].astype(jnp.float32), tile)
    o_ref[2 * BK : ROWS, :] = tile.astype(jnp.bfloat16)


def attend_kernel(nblocks, first, last, qo_ref, qz_ref, qc_ref, qd_ref, *rest):
    blocks, rest = rest[:nblocks], list(rest[nblocks:])
    accin_ref, min_ref = (None, None) if first else (rest.pop(0), rest.pop(0))
    out_ref = rest.pop(0) if last else None
    acc_ref, m_ref, q_ref, off_ref, qp, qt, kp = rest
    core = lax.axis_index("blk") % NC
    side = lax.axis_index("col") % 2
    pos = []
    for t in range(4):
        q_ref[t, 0:128, :] = qo_ref[t * 128 : (t + 1) * 128, :]
        q_ref[t, 128:256, :] = qz_ref[t * 128 : (t + 1) * 128, :]
        q_ref[4 + t, 0:128, :] = qc_ref[t * 128 : (t + 1) * 128, :]
        q_ref[4 + t, 128:256, :] = qd_ref[t * 128 : (t + 1) * 128, :]
    for ref in (qo_ref, qc_ref):
        for t in range(4):
            pos.append(scalar_of(ref[512 + t : 513 + t, :]))
    for j in range(NQ):
        rank = jnp.int32(0)
        for i in range(NQ):
            if i != j:
                rank = rank + (pos[i] < pos[j]).astype(jnp.int32)
        qp[rank] = pos[j]
        qt[rank] = jnp.int32(j)
    for n, blk in enumerate(blocks):
        for j in range(NST):
            kp[n * NST + j] = scalar_of(blk[2 * BK + j : 2 * BK + j + 1, :])
    if first:
        r = lax.broadcasted_iota(jnp.int32, (SUB, 256), 0)
        lane = lax.broadcasted_iota(jnp.int32, (SUB, 256), 1)
        off = (r // 32) * 64 + side * 32 + r % 32 - lane % 128
        off_ref[0] = jnp.zeros((SUB, 256), jnp.float32)
        off_ref[1] = jnp.where(off <= 0, 0.0, MASKED)
        acc_ref[...] = jnp.zeros_like(acc_ref)
        m_ref[...] = jnp.full(m_ref.shape, EMPTY, jnp.float32)
    else:
        acc_ref[...] = accin_ref[...]
        m_ref[...] = min_ref[...]
    ones = jnp.ones((16, BK), jnp.bfloat16)

    def scores(t, keys):
        return [
            lax.dot_general(blk[0:keys, :], q_ref[t], (((1,), (1,)), ((), ())), preferred_element_type=jnp.float32)
            for blk in blocks
        ]

    def local(qpos, raw, keys):
        parts = []
        top = None
        for n, s in enumerate(raw):
            runs = []
            for j in range(keys // SUB):
                run = s[j * SUB : (j + 1) * SUB, :]
                kpos = kp[n * NST + j]
                if first:
                    run = run + off_ref[(kpos == qpos).astype(jnp.int32)]
                hidden = jnp.where(kpos <= qpos, 0.0, MASKED).astype(jnp.float32)
                high = jnp.max(run.reshape(SUB // 8, 8, 256), axis=0) * C2 + hidden
                top = high if top is None else jnp.maximum(top, high)
                runs.append((run, hidden))
            parts.append(runs)
        top = jnp.maximum(jnp.max(top, axis=0, keepdims=True), EMPTY)
        mixed = None
        for runs, blk in zip(parts, blocks):
            p = jnp.concatenate([jnp.exp2(run * C2 + (hidden - top)) for run, hidden in runs], axis=0)
            vt = jnp.concatenate(
                [blk[BK + i * DH : BK + (i + 1) * DH, :] for i in range(keys // DH)], axis=1
            )
            vt = jnp.concatenate([vt, ones[:, 0:keys]], axis=0)
            part = jnp.dot(vt, p.astype(jnp.bfloat16), preferred_element_type=jnp.float32)
            mixed = part if mixed is None else mixed + part
        return top, mixed

    size = 2

    def together(i, keys):
        raws = [scores(qt[size * i + k], keys) for k in range(size)]
        found = [(qt[size * i + k],) + local(qp[size * i + k], raws[k], keys) for k in range(size)]
        for t, top, mixed in found:
            old = m_ref[t, 0:1, :]
            new = jnp.maximum(old, top)
            acc_ref[t] = acc_ref[t] * jnp.exp2(old - new) + mixed * jnp.exp2(top - new)
            m_ref[t] = jnp.broadcast_to(new, (8, 256))

    def group(i, carry):
        far = qp[size * i + size - 1]
        need = jnp.int32(0)
        for n in range(nblocks):
            seen = jnp.int32(0)
            for j in (0, 4, 6):
                seen = seen + (kp[n * NST + j] <= far).astype(jnp.int32)
            need = jnp.maximum(need, seen)
        for level, keys in ((1, 4 * SUB), (2, 6 * SUB), (3, 8 * SUB)):

            @pl.when(need == level)
            def _(keys=keys):
                together(i, keys)

        return carry

    lax.fori_loop(0, NQ // size, group, 0)
    if last:
        partial(core, side, acc_ref, m_ref, out_ref)


def partial(core, side, acc_ref, m_ref, o_ref):
    for dc in range(2):
        for dz in range(2):
            member = (core + dc - 2 * core * dc) * 2 + (side + dz - 2 * side * dz)
            rows = []
            for t in range(4):
                st = dc * 4 + t
                lanes = slice(dz * 128, dz * 128 + 128)
                total = acc_ref[st, 128:129, lanes]
                top = m_ref[st, 0:1, lanes]
                seen = total > 0.0
                inv = jnp.where(seen, 1.0 / jnp.where(seen, total, 1.0), 0.0)
                o_ref[member, t * 128 : (t + 1) * 128, :] = (acc_ref[st, 0:128, lanes] * inv).T.astype(jnp.bfloat16)
                rows.append(jnp.where(seen, top + jnp.log2(jnp.where(seen, total, 1.0)), EMPTY))
            lse = jnp.concatenate(rows, axis=0)
            hi = lse.astype(jnp.bfloat16).astype(jnp.float32)
            mid = (lse - hi).astype(jnp.bfloat16).astype(jnp.float32)
            low = lse - hi - mid
            o_ref[member, 512:528, :] = jnp.concatenate(
                [hi, mid, low, jnp.zeros((4, 128), jnp.float32)], axis=0
            ).astype(jnp.bfloat16)


def merge_kernel(i_ref, o_ref, l_ref):
    lses = []
    for m in range(4):
        tile = i_ref[m, 512:528, :].astype(jnp.float32)
        lses.append(tile[0:4] + tile[4:8] + tile[8:12])
    top = jnp.maximum(jnp.maximum(lses[0], lses[1]), jnp.maximum(lses[2], lses[3]))
    ws = [jnp.exp2(x - top) for x in lses]
    total = ws[0] + ws[1] + ws[2] + ws[3]
    l_ref[...] = (top + jnp.log2(total)) * LN2
    inv = 1.0 / total
    for t in range(4):
        out = None
        for m in range(4):
            w = jnp.broadcast_to((ws[m] * inv)[t : t + 1, :], (128, 128)).T
            part = i_ref[m, t * 128 : (t + 1) * 128, :].astype(jnp.float32) * w
            out = part if out is None else out + part
        o_ref[t * 128 : (t + 1) * 128, :] = out


def body(queries, keys, values, positions):
    bf, f32 = jnp.bfloat16, jnp.float32
    core = lax.axis_index("blk") % NC

    packed, qo = call(
        pack_kernel,
        (jax.ShapeDtypeStruct((16, 72, DH), bf), jax.ShapeDtypeStruct((528, DH), bf)),
        "hhhh",
        scratch=[
            SM((512,), jnp.int32),
            VM((32, HK * DH), bf),
            VM((32, HK * DH), bf),
            pltpu.SemaphoreType.DMA((4,)),
        ],
        name="pack",
    )(*[pltpu.with_memory_space_constraint(a, pltpu.HBM) for a in (positions, keys, values, queries)])
    got = lax.all_to_all(packed, ("blk", "col"), 0, 0, axis_index_groups=KV_GROUPS, tiled=False)
    qz, qc = send(qo, ZPAIR), send(qo, CORE)
    qd = send(qz, CORE)
    qs = (qo, qz, qc, qd)
    own = call(
        prep_kernel,
        jax.ShapeDtypeStruct((ROWS, DH), bf),
        "v",
        scratch=[VM((BK, DH), f32), SM((NST,), jnp.int32)],
        name="prep",
    )(got)

    up, down = [send(own, UP)], [send(own, DOWN)]
    for step in range(2):
        up.append(send(up[-1], UP))
        down.append(send(down[-1], DOWN))
    far = send(jnp.where(core == 0, up[1], down[1]), LAST)

    acc = jax.ShapeDtypeStruct((NQ, 144, 256), f32)
    top = jax.ShapeDtypeStruct((NQ, 8, 256), f32)

    def attend(blocks, carry, last=False):
        n = len(blocks)
        first = carry is None
        kernel = lambda *refs: attend_kernel(n, first, last, *refs)
        scratch = [
            VM((NQ, 256, DH), bf),
            VM((2, SUB, 256), f32),
            SM((NQ,), jnp.int32),
            SM((NQ,), jnp.int32),
            SM((n * NST,), jnp.int32),
        ]
        if last:
            scratch = [VM(acc.shape, f32), VM(top.shape, f32)] + scratch
        args = qs + tuple(blocks) + (() if first else carry)
        return call(
            kernel,
            jax.ShapeDtypeStruct((4, 528, DH), bf) if last else (acc, top),
            "v" * len(args),
            scratch=scratch,
            alias=None if first or last else {4 + n: 0, 5 + n: 1},
            flops=n * 2_000_000_000,
            name=f"attend{n}",
        )(*args)

    carry = attend([own], None)
    carry = attend([up[0], down[0]], carry)
    carry = attend([up[1], down[1]], carry)
    part = attend([up[2], down[2], far], carry, last=True)
    parts = lax.all_to_all(part, ("blk", "col"), 0, 0, axis_index_groups=OUT_GROUPS, tiled=False)
    attended, lognorm = call(
        merge_kernel,
        (jax.ShapeDtypeStruct((512, DH), f32), jax.ShapeDtypeStruct((4, 128), f32)),
        "v",
        name="merge",
    )(parts)
    return attended, lognorm.reshape(512, 1)


def solution(mesh):
    placed = (P("blk", "col"), P(("blk", "col"), None), P(("blk", "col"), None), P("blk"))
    return jax.shard_map(
        body,
        mesh=mesh,
        in_specs=placed,
        out_specs=(P("blk", "col"), P("blk", "col")),
        check_vma=False,
    )
```

```python
import math

import jax
import jax.numpy as jnp
from jax import lax
from jax.experimental import pallas as pl
from jax.experimental.pallas import tpu as pltpu
from jax.sharding import PartitionSpec as P

HQ = 16
HK = 4
DH = 128
STRIPE = 128
NY, NZH, NC, NX, NZL = 8, 2, 2, 4, 4
SUB = 64
NST = 8
BK = NST * SUB
ROWS = 2 * BK + 16
NQ = 8
C2 = math.log2(math.e) / math.sqrt(DH)
LN2 = math.log(2.0)
MASKED = -1e30
EMPTY = -1e29
VM = pltpu.VMEM
SM = pltpu.SMEM


def flat_groups(key):
    found = {}
    for b in range(NY * NZH * NC):
        for c in range(NX * NZL):
            k = key(b // 4, (b // 2) % 2, b % 2, c // 4, c % 4)
            found.setdefault(k, []).append(b * NX * NZL + c)
    return list(found.values())


KV_GROUPS = flat_groups(lambda y, zh, c, x, zl: (y, c, zl % 2))
OUT_GROUPS = flat_groups(lambda y, zh, c, x, zl: (y, zh, x, zl // 2))


def pairs(move):
    out = []
    for b in range(NY * NZH * NC):
        for c in range(NX * NZL):
            y, zh, co, x, zl = move(b // 4, (b // 2) % 2, b % 2, c // 4, c % 4)
            out.append((b * 16 + c, ((y % NY) * 4 + zh * 2 + co) * 16 + x * 4 + zl))
    return out


UP = pairs(lambda y, zh, c, x, zl: (y + 1, zh, c, x, zl))
DOWN = pairs(lambda y, zh, c, x, zl: (y - 1, zh, c, x, zl))
LAST = pairs(lambda y, zh, c, x, zl: (y + 1 - 2 * c, zh, c, x, zl))
CORE = pairs(lambda y, zh, c, x, zl: (y, zh, 1 - c, x, zl))
ZPAIR = pairs(lambda y, zh, c, x, zl: (y, zh, c, x, zl ^ 1))


def send(value, perm):
    return lax.ppermute(value, ("blk", "col"), perm)


def call(kernel, out, in_spaces, scratch=(), alias=None, name=None, flops=0):
    vm = pl.BlockSpec(memory_space=VM)
    sm = pl.BlockSpec(memory_space=SM)
    return pl.pallas_call(
        kernel,
        out_shape=out,
        in_specs=[{"s": sm, "v": vm, "h": pl.BlockSpec(memory_space=pltpu.HBM)}[s] for s in in_spaces],
        out_specs=jax.tree.map(lambda _: vm, out),
        scratch_shapes=list(scratch),
        input_output_aliases=alias or {},
        name=name,
        cost_estimate=pl.CostEstimate(flops=flops, transcendentals=0, bytes_accessed=0) if flops else None,
        compiler_params=pltpu.CompilerParams(vmem_limit_bytes=40 * 1024 * 1024),
    )


def pack_kernel(pos_hbm, k_hbm, v_hbm, q_hbm, o_ref, q_ref, pos, k_ref, v_ref, sems):
    copies = [
        pltpu.make_async_copy(src, dst, sems.at[i])
        for i, (src, dst) in enumerate(
            [(pos_hbm, pos), (k_hbm, k_ref), (v_hbm, v_ref), (q_hbm, q_ref.at[pl.ds(0, 512)])]
        )
    ]
    for c in copies:
        c.start()
    copies[0].wait()
    x = lax.axis_index("col") // NZL
    mine = pos[pl.multiple_of(x * STRIPE, STRIPE)] // STRIPE
    tile = jnp.full((8, DH), mine.astype(jnp.float32), jnp.float32).astype(jnp.bfloat16)
    for m in range(16):
        o_ref[m, 64:72, :] = tile
    row = lax.broadcasted_iota(jnp.int32, (16, DH), 0)
    tile = jnp.zeros((16, DH), jnp.float32)
    for r in range(4):
        tile = jnp.where(row == r, (pos[r * STRIPE] // STRIPE).astype(jnp.float32), tile)
    q_ref[512:528, :] = tile.astype(jnp.bfloat16)
    for at, ref, c in ((0, k_ref, copies[1]), (32, v_ref, copies[2])):
        c.wait()
        for m in range(16):
            head = (m // 2) % 4
            o_ref[m, at : at + 32, :] = ref[:, head * DH : (head + 1) * DH]
    copies[3].wait()


def scalar_of(row):
    return jnp.max(row.astype(jnp.float32)).astype(jnp.int32)


def prep_kernel(r_ref, o_ref, v_scr, p_scr):
    pos = []
    for j in range(NST):
        m = (j // 4) * 8 + (j % 4) * 2
        pos.append(scalar_of(r_ref[m, 64:65, :]))
    for j in range(NST):
        rank = jnp.int32(0)
        for i in range(NST):
            if i != j:
                rank = rank + (pos[i] < pos[j]).astype(jnp.int32)
        p_scr[rank] = pos[j]
        m = (j // 4) * 8 + (j % 4) * 2
        at = pl.multiple_of(rank * SUB, SUB)
        kk = jnp.concatenate([r_ref[m, 0:32, :], r_ref[m + 1, 0:32, :]], axis=0)
        vv = jnp.concatenate([r_ref[m, 32:64, :], r_ref[m + 1, 32:64, :]], axis=0)
        o_ref[pl.ds(at, SUB), :] = kk
        v_scr[pl.ds(at, SUB), :] = vv.astype(jnp.float32)
    for t in range(BK // DH):
        o_ref[BK + t * DH : BK + (t + 1) * DH, :] = v_scr[t * DH : (t + 1) * DH, :].T.astype(jnp.bfloat16)
    row = lax.broadcasted_iota(jnp.int32, (16, DH), 0)
    tile = jnp.zeros((16, DH), jnp.float32)
    for r in range(NST):
        tile = jnp.where(row == r, p_scr[r].astype(jnp.float32), tile)
    o_ref[2 * BK : ROWS, :] = tile.astype(jnp.bfloat16)


def attend_kernel(nblocks, first, last, qo_ref, qz_ref, qc_ref, qd_ref, *rest):
    blocks, rest = rest[:nblocks], list(rest[nblocks:])
    accin_ref, min_ref = (None, None) if first else (rest.pop(0), rest.pop(0))
    out_ref = rest.pop(0) if last else None
    acc_ref, m_ref, q_ref, off_ref, qp, qt, kp = rest
    core = lax.axis_index("blk") % NC
    side = lax.axis_index("col") % 2
    pos = []
    for t in range(4):
        q_ref[t, 0:128, :] = qo_ref[t * 128 : (t + 1) * 128, :]
        q_ref[t, 128:256, :] = qz_ref[t * 128 : (t + 1) * 128, :]
        q_ref[4 + t, 0:128, :] = qc_ref[t * 128 : (t + 1) * 128, :]
        q_ref[4 + t, 128:256, :] = qd_ref[t * 128 : (t + 1) * 128, :]
    for ref in (qo_ref, qc_ref):
        for t in range(4):
            pos.append(scalar_of(ref[512 + t : 513 + t, :]))
    for j in range(NQ):
        rank = jnp.int32(0)
        for i in range(NQ):
            if i != j:
                rank = rank + (pos[i] < pos[j]).astype(jnp.int32)
        qp[rank] = pos[j]
        qt[rank] = jnp.int32(j)
    for n, blk in enumerate(blocks):
        for j in range(NST):
            kp[n * NST + j] = scalar_of(blk[2 * BK + j : 2 * BK + j + 1, :])
    if first:
        r = lax.broadcasted_iota(jnp.int32, (SUB, 256), 0)
        lane = lax.broadcasted_iota(jnp.int32, (SUB, 256), 1)
        off = (r // 32) * 64 + side * 32 + r % 32 - lane % 128
        off_ref[0] = jnp.zeros((SUB, 256), jnp.float32)
        off_ref[1] = jnp.where(off <= 0, 0.0, MASKED)
        acc_ref[...] = jnp.zeros_like(acc_ref)
        m_ref[...] = jnp.full(m_ref.shape, EMPTY, jnp.float32)
    else:
        acc_ref[...] = accin_ref[...]
        m_ref[...] = min_ref[...]
    ones = jnp.ones((16, BK), jnp.bfloat16)

    def scores(t, keys):
        return [
            lax.dot_general(blk[0:keys, :], q_ref[t], (((1,), (1,)), ((), ())), preferred_element_type=jnp.float32)
            for blk in blocks
        ]

    def local(qpos, raw, keys):
        parts = []
        top = None
        for n, s in enumerate(raw):
            runs = []
            for j in range(keys // SUB):
                run = s[j * SUB : (j + 1) * SUB, :]
                kpos = kp[n * NST + j]
                if first:
                    run = run + off_ref[(kpos == qpos).astype(jnp.int32)]
                hidden = jnp.where(kpos <= qpos, 0.0, MASKED).astype(jnp.float32)
                high = jnp.max(run.reshape(SUB // 8, 8, 256), axis=0) * C2 + hidden
                top = high if top is None else jnp.maximum(top, high)
                runs.append((run, hidden))
            parts.append(runs)
        top = jnp.maximum(jnp.max(top, axis=0, keepdims=True), EMPTY)
        mixed = None
        for runs, blk in zip(parts, blocks):
            p = jnp.concatenate([jnp.exp2(run * C2 + (hidden - top)) for run, hidden in runs], axis=0)
            vt = jnp.concatenate(
                [blk[BK + i * DH : BK + (i + 1) * DH, :] for i in range(keys // DH)], axis=1
            )
            vt = jnp.concatenate([vt, ones[:, 0:keys]], axis=0)
            part = jnp.dot(vt, p.astype(jnp.bfloat16), preferred_element_type=jnp.float32)
            mixed = part if mixed is None else mixed + part
        return top, mixed

    size = 2

    def together(i, keys):
        raws = [scores(qt[size * i + k], keys) for k in range(size)]
        found = [(qt[size * i + k],) + local(qp[size * i + k], raws[k], keys) for k in range(size)]
        for t, top, mixed in found:
            old = m_ref[t, 0:1, :]
            new = jnp.maximum(old, top)
            acc_ref[t] = acc_ref[t] * jnp.exp2(old - new) + mixed * jnp.exp2(top - new)
            m_ref[t] = jnp.broadcast_to(new, (8, 256))

    def group(i, carry):
        far = qp[size * i + size - 1]
        need = jnp.int32(0)
        for n in range(nblocks):
            seen = jnp.int32(0)
            for j in (0, 2, 4, 6):
                seen = seen + (kp[n * NST + j] <= far).astype(jnp.int32)
            need = jnp.maximum(need, seen)
        for level, keys in ((1, 2 * SUB), (2, 4 * SUB), (3, 6 * SUB), (4, 8 * SUB)):

            @pl.when(need == level)
            def _(keys=keys):
                together(i, keys)

        return carry

    lax.fori_loop(0, NQ // size, group, 0)
    if last:
        partial(core, side, acc_ref, m_ref, out_ref)


def partial(core, side, acc_ref, m_ref, o_ref):
    for dc in range(2):
        for dz in range(2):
            member = (core + dc - 2 * core * dc) * 2 + (side + dz - 2 * side * dz)
            rows = []
            for t in range(4):
                st = dc * 4 + t
                lanes = slice(dz * 128, dz * 128 + 128)
                total = acc_ref[st, 128:129, lanes]
                top = m_ref[st, 0:1, lanes]
                seen = total > 0.0
                inv = jnp.where(seen, 1.0 / jnp.where(seen, total, 1.0), 0.0)
                o_ref[member, t * 128 : (t + 1) * 128, :] = (acc_ref[st, 0:128, lanes] * inv).T.astype(jnp.bfloat16)
                rows.append(jnp.where(seen, top + jnp.log2(jnp.where(seen, total, 1.0)), EMPTY))
            lse = jnp.concatenate(rows, axis=0)
            hi = lse.astype(jnp.bfloat16).astype(jnp.float32)
            mid = (lse - hi).astype(jnp.bfloat16).astype(jnp.float32)
            low = lse - hi - mid
            o_ref[member, 512:528, :] = jnp.concatenate(
                [hi, mid, low, jnp.zeros((4, 128), jnp.float32)], axis=0
            ).astype(jnp.bfloat16)


def merge_kernel(i_ref, o_ref, l_ref):
    lses = []
    for m in range(4):
        tile = i_ref[m, 512:528, :].astype(jnp.float32)
        lses.append(tile[0:4] + tile[4:8] + tile[8:12])
    top = jnp.maximum(jnp.maximum(lses[0], lses[1]), jnp.maximum(lses[2], lses[3]))
    ws = [jnp.exp2(x - top) for x in lses]
    total = ws[0] + ws[1] + ws[2] + ws[3]
    l_ref[...] = (top + jnp.log2(total)) * LN2
    inv = 1.0 / total
    for t in range(4):
        out = None
        for m in range(4):
            w = jnp.broadcast_to((ws[m] * inv)[t : t + 1, :], (128, 128)).T
            part = i_ref[m, t * 128 : (t + 1) * 128, :].astype(jnp.float32) * w
            out = part if out is None else out + part
        o_ref[t * 128 : (t + 1) * 128, :] = out


def body(queries, keys, values, positions):
    bf, f32 = jnp.bfloat16, jnp.float32
    core = lax.axis_index("blk") % NC

    packed, qo = call(
        pack_kernel,
        (jax.ShapeDtypeStruct((16, 72, DH), bf), jax.ShapeDtypeStruct((528, DH), bf)),
        "hhhh",
        scratch=[
            SM((512,), jnp.int32),
            VM((32, HK * DH), bf),
            VM((32, HK * DH), bf),
            pltpu.SemaphoreType.DMA((4,)),
        ],
        name="pack",
    )(*[pltpu.with_memory_space_constraint(a, pltpu.HBM) for a in (positions, keys, values, queries)])
    got = lax.all_to_all(packed, ("blk", "col"), 0, 0, axis_index_groups=KV_GROUPS, tiled=False)
    qz, qc = send(qo, ZPAIR), send(qo, CORE)
    qd = send(qz, CORE)
    qs = (qo, qz, qc, qd)
    own = call(
        prep_kernel,
        jax.ShapeDtypeStruct((ROWS, DH), bf),
        "v",
        scratch=[VM((BK, DH), f32), SM((NST,), jnp.int32)],
        name="prep",
    )(got)

    up, down = [send(own, UP)], [send(own, DOWN)]
    for step in range(2):
        up.append(send(up[-1], UP))
        down.append(send(down[-1], DOWN))
    far = send(jnp.where(core == 0, up[2], down[2]), LAST)

    acc = jax.ShapeDtypeStruct((NQ, 144, 256), f32)
    top = jax.ShapeDtypeStruct((NQ, 8, 256), f32)

    def attend(blocks, carry, last=False):
        n = len(blocks)
        first = carry is None
        kernel = lambda *refs: attend_kernel(n, first, last, *refs)
        scratch = [
            VM((NQ, 256, DH), bf),
            VM((2, SUB, 256), f32),
            SM((NQ,), jnp.int32),
            SM((NQ,), jnp.int32),
            SM((n * NST,), jnp.int32),
        ]
        if last:
            scratch = [VM(acc.shape, f32), VM(top.shape, f32)] + scratch
        args = qs + tuple(blocks) + (() if first else carry)
        return call(
            kernel,
            jax.ShapeDtypeStruct((4, 528, DH), bf) if last else (acc, top),
            "v" * len(args),
            scratch=scratch,
            alias=None if first or last else {4 + n: 0, 5 + n: 1},
            flops=n * 2_000_000_000,
            name=f"attend{n}",
        )(*args)

    carry = attend([own], None)
    carry = attend([up[0], down[0]], carry)
    carry = attend([up[1], down[1]], carry)
    carry = attend([up[2], down[2]], carry)
    part = attend([far], carry, last=True)
    parts = lax.all_to_all(part, ("blk", "col"), 0, 0, axis_index_groups=OUT_GROUPS, tiled=False)
    attended, lognorm = call(
        merge_kernel,
        (jax.ShapeDtypeStruct((512, DH), f32), jax.ShapeDtypeStruct((4, 128), f32)),
        "v",
        name="merge",
    )(parts)
    return attended, lognorm.reshape(512, 1)


def solution(mesh):
    placed = (P("blk", "col"), P(("blk", "col"), None), P(("blk", "col"), None), P("blk"))
    return jax.shard_map(
        body,
        mesh=mesh,
        in_specs=placed,
        out_specs=(P("blk", "col"), P("blk", "col")),
        check_vma=False,
    )
```

```python
import math

import jax
import jax.numpy as jnp
from jax import lax
from jax.experimental import pallas as pl
from jax.experimental.pallas import tpu as pltpu
from jax.sharding import PartitionSpec as P


HK = 4
DH = 128
STRIPE = 128
NY, NZH, NC, NX, NZL = 8, 2, 2, 4, 4
SUB = 64
NST = 8
BK = NST * SUB
ROWS = 2 * BK + 16
NQ = 8
C2 = math.log2(math.e) / math.sqrt(DH)
LN2 = math.log(2.0)
MASKED = -1e30
EMPTY = -1e29
VM = pltpu.VMEM
SM = pltpu.SMEM


def flat_groups(key):
    found = {}
    for b in range(NY * NZH * NC):
        for c in range(NX * NZL):
            k = key(b // 4, (b // 2) % 2, b % 2, c // 4, c % 4)
            found.setdefault(k, []).append(b * NX * NZL + c)
    return list(found.values())


KV_GROUPS = flat_groups(lambda y, zh, c, x, zl: (y, c, zl % 2))
OUT_GROUPS = flat_groups(lambda y, zh, c, x, zl: (y, zh, x, zl // 2))


def pairs(move):
    out = []
    for b in range(NY * NZH * NC):
        for c in range(NX * NZL):
            y, zh, co, x, zl = move(b // 4, (b // 2) % 2, b % 2, c // 4, c % 4)
            out.append((b * 16 + c, ((y % NY) * 4 + zh * 2 + co) * 16 + x * 4 + zl))
    return out


UP = pairs(lambda y, zh, c, x, zl: (y + 1, zh, c, x, zl))
DOWN = pairs(lambda y, zh, c, x, zl: (y - 1, zh, c, x, zl))
LAST = pairs(lambda y, zh, c, x, zl: (y + 2 - 4 * c, zh, c, x, zl))
CORE = pairs(lambda y, zh, c, x, zl: (y, zh, 1 - c, x, zl))
ZPAIR = pairs(lambda y, zh, c, x, zl: (y, zh, c, x, zl ^ 1))


def send(value, perm):
    return lax.ppermute(value, ("blk", "col"), perm)


def call(kernel, out, in_spaces, scratch=(), alias=None, flops=0):
    vm = pl.BlockSpec(memory_space=VM)
    sm = pl.BlockSpec(memory_space=SM)
    return pl.pallas_call(
        kernel,
        out_shape=out,
        in_specs=[{"s": sm, "v": vm, "h": pl.BlockSpec(memory_space=pltpu.HBM)}[s] for s in in_spaces],
        out_specs=jax.tree.map(lambda _: vm, out),
        scratch_shapes=list(scratch),
        input_output_aliases=alias or {},
        cost_estimate=pl.CostEstimate(flops=flops, transcendentals=0, bytes_accessed=0) if flops else None,
        compiler_params=pltpu.CompilerParams(vmem_limit_bytes=40 * 1024 * 1024),
    )


def pack_kernel(pos_hbm, k_hbm, v_hbm, q_hbm, o_ref, q_ref, pos, k_ref, v_ref, sems):
    copies = [
        pltpu.make_async_copy(src, dst, sems.at[i])
        for i, (src, dst) in enumerate(
            [(pos_hbm, pos), (k_hbm, k_ref), (v_hbm, v_ref), (q_hbm, q_ref.at[pl.ds(0, 512)])]
        )
    ]
    for c in copies:
        c.start()
    copies[0].wait()
    x = lax.axis_index("col") // NZL
    mine = pos[pl.multiple_of(x * STRIPE, STRIPE)] // STRIPE
    tile = jnp.full((8, DH), mine.astype(jnp.float32), jnp.float32).astype(jnp.bfloat16)
    for m in range(16):
        o_ref[m, 64:72, :] = tile
    row = lax.broadcasted_iota(jnp.int32, (16, DH), 0)
    tile = jnp.zeros((16, DH), jnp.float32)
    for r in range(4):
        tile = jnp.where(row == r, (pos[r * STRIPE] // STRIPE).astype(jnp.float32), tile)
    q_ref[512:528, :] = tile.astype(jnp.bfloat16)
    for at, ref, c in ((0, k_ref, copies[1]), (32, v_ref, copies[2])):
        c.wait()
        for m in range(16):
            head = (m // 2) % 4
            o_ref[m, at : at + 32, :] = ref[:, head * DH : (head + 1) * DH]
    copies[3].wait()


def scalar_of(row):
    return jnp.max(row.astype(jnp.float32)).astype(jnp.int32)


def prep_kernel(r_ref, o_ref, v_scr, p_scr):
    pos = []
    for j in range(NST):
        m = (j // 4) * 8 + (j % 4) * 2
        pos.append(scalar_of(r_ref[m, 64:65, :]))
    for j in range(NST):
        rank = jnp.int32(0)
        for i in range(NST):
            if i != j:
                rank = rank + (pos[i] < pos[j]).astype(jnp.int32)
        p_scr[rank] = pos[j]
        m = (j // 4) * 8 + (j % 4) * 2
        at = pl.multiple_of(rank * SUB, SUB)
        kk = jnp.concatenate([r_ref[m, 0:32, :], r_ref[m + 1, 0:32, :]], axis=0)
        vv = jnp.concatenate([r_ref[m, 32:64, :], r_ref[m + 1, 32:64, :]], axis=0)
        o_ref[pl.ds(at, SUB), :] = kk
        v_scr[pl.ds(at, SUB), :] = vv.astype(jnp.float32)
    for t in range(BK // DH):
        o_ref[BK + t * DH : BK + (t + 1) * DH, :] = v_scr[t * DH : (t + 1) * DH, :].T.astype(jnp.bfloat16)
    row = lax.broadcasted_iota(jnp.int32, (16, DH), 0)
    tile = jnp.zeros((16, DH), jnp.float32)
    for r in range(NST):
        tile = jnp.where(row == r, p_scr[r].astype(jnp.float32), tile)
    o_ref[2 * BK : ROWS, :] = tile.astype(jnp.bfloat16)


def attend_kernel(nblocks, first, last, qo_ref, qz_ref, qc_ref, qd_ref, *rest):
    blocks, rest = rest[:nblocks], list(rest[nblocks:])
    accin_ref, min_ref = (None, None) if first else (rest.pop(0), rest.pop(0))
    out_ref = rest.pop(0) if last else None
    acc_ref, m_ref, q_ref, off_ref, qp, qt, kp = rest
    core = lax.axis_index("blk") % NC
    side = lax.axis_index("col") % 2
    pos = []
    for t in range(4):
        q_ref[t, 0:128, :] = qo_ref[t * 128 : (t + 1) * 128, :]
        q_ref[t, 128:256, :] = qz_ref[t * 128 : (t + 1) * 128, :]
        q_ref[4 + t, 0:128, :] = qc_ref[t * 128 : (t + 1) * 128, :]
        q_ref[4 + t, 128:256, :] = qd_ref[t * 128 : (t + 1) * 128, :]
    for ref in (qo_ref, qc_ref):
        for t in range(4):
            pos.append(scalar_of(ref[512 + t : 513 + t, :]))
    for j in range(NQ):
        rank = jnp.int32(0)
        for i in range(NQ):
            if i != j:
                rank = rank + (pos[i] < pos[j]).astype(jnp.int32)
        qp[rank] = pos[j]
        qt[rank] = jnp.int32(j)
    for n, blk in enumerate(blocks):
        for j in range(NST):
            kp[n * NST + j] = scalar_of(blk[2 * BK + j : 2 * BK + j + 1, :])
    if first:
        r = lax.broadcasted_iota(jnp.int32, (SUB, 256), 0)
        lane = lax.broadcasted_iota(jnp.int32, (SUB, 256), 1)
        off = (r // 32) * 64 + side * 32 + r % 32 - lane % 128
        off_ref[0] = jnp.zeros((SUB, 256), jnp.float32)
        off_ref[1] = jnp.where(off <= 0, 0.0, MASKED)
        acc_ref[...] = jnp.zeros_like(acc_ref)
        m_ref[...] = jnp.full(m_ref.shape, EMPTY, jnp.float32)
    else:
        acc_ref[...] = accin_ref[...]
        m_ref[...] = min_ref[...]
    ones = jnp.ones((16, BK), jnp.bfloat16)

    def scores(t, keys):
        return [
            lax.dot_general(blk[0:keys, :], q_ref[t], (((1,), (1,)), ((), ())), preferred_element_type=jnp.float32)
            for blk in blocks
        ]

    def local(qpos, raw, keys):
        parts = []
        top = None
        for n, s in enumerate(raw):
            runs = []
            for j in range(keys // SUB):
                run = s[j * SUB : (j + 1) * SUB, :]
                kpos = kp[n * NST + j]
                if first:
                    run = run + off_ref[(kpos == qpos).astype(jnp.int32)]
                hidden = jnp.where(kpos <= qpos, 0.0, MASKED).astype(jnp.float32)
                high = jnp.max(run.reshape(SUB // 8, 8, 256), axis=0) * C2 + hidden
                top = high if top is None else jnp.maximum(top, high)
                runs.append((run, hidden))
            parts.append(runs)
        top = jnp.maximum(jnp.max(top, axis=0, keepdims=True), EMPTY)
        mixed = None
        for runs, blk in zip(parts, blocks):
            p = jnp.concatenate([jnp.exp2(run * C2 + (hidden - top)) for run, hidden in runs], axis=0)
            vt = jnp.concatenate(
                [blk[BK + i * DH : BK + (i + 1) * DH, :] for i in range(keys // DH)], axis=1
            )
            vt = jnp.concatenate([vt, ones[:, 0:keys]], axis=0)
            part = jnp.dot(vt, p.astype(jnp.bfloat16), preferred_element_type=jnp.float32)
            mixed = part if mixed is None else mixed + part
        return top, mixed

    size = 2

    def together(i, keys):
        raws = [scores(qt[size * i + k], keys) for k in range(size)]
        found = [(qt[size * i + k],) + local(qp[size * i + k], raws[k], keys) for k in range(size)]
        for t, top, mixed in found:
            old = m_ref[t, 0:1, :]
            new = jnp.maximum(old, top)
            acc_ref[t] = acc_ref[t] * jnp.exp2(old - new) + mixed * jnp.exp2(top - new)
            m_ref[t] = jnp.broadcast_to(new, (8, 256))

    def group(i, carry):
        far = qp[size * i + size - 1]
        need = jnp.int32(0)
        for n in range(nblocks):
            seen = jnp.int32(0)
            for j in (0, 2, 4, 6):
                seen = seen + (kp[n * NST + j] <= far).astype(jnp.int32)
            need = jnp.maximum(need, seen)
        for level, keys in ((1, 2 * SUB), (2, 4 * SUB), (3, 6 * SUB), (4, 8 * SUB)):

            @pl.when(need == level)
            def _(keys=keys):
                together(i, keys)

        return carry

    lax.fori_loop(0, NQ // size, group, 0)
    if last:
        partial(core, side, acc_ref, m_ref, out_ref)


def partial(core, side, acc_ref, m_ref, o_ref):
    for dc in range(2):
        for dz in range(2):
            member = (core + dc - 2 * core * dc) * 2 + (side + dz - 2 * side * dz)
            rows = []
            for t in range(4):
                st = dc * 4 + t
                lanes = slice(dz * 128, dz * 128 + 128)
                total = acc_ref[st, 128:129, lanes]
                top = m_ref[st, 0:1, lanes]
                seen = total > 0.0
                inv = jnp.where(seen, 1.0 / jnp.where(seen, total, 1.0), 0.0)
                o_ref[member, t * 128 : (t + 1) * 128, :] = (acc_ref[st, 0:128, lanes] * inv).T.astype(jnp.bfloat16)
                rows.append(jnp.where(seen, top + jnp.log2(jnp.where(seen, total, 1.0)), EMPTY))
            lse = jnp.concatenate(rows, axis=0)
            hi = lse.astype(jnp.bfloat16).astype(jnp.float32)
            mid = (lse - hi).astype(jnp.bfloat16).astype(jnp.float32)
            low = lse - hi - mid
            o_ref[member, 512:528, :] = jnp.concatenate(
                [hi, mid, low, jnp.zeros((4, 128), jnp.float32)], axis=0
            ).astype(jnp.bfloat16)


def merge_kernel(i_ref, o_ref, l_ref):
    lses = []
    for m in range(4):
        tile = i_ref[m, 512:528, :].astype(jnp.float32)
        lses.append(tile[0:4] + tile[4:8] + tile[8:12])
    top = jnp.maximum(jnp.maximum(lses[0], lses[1]), jnp.maximum(lses[2], lses[3]))
    ws = [jnp.exp2(x - top) for x in lses]
    total = ws[0] + ws[1] + ws[2] + ws[3]
    l_ref[...] = (top + jnp.log2(total)) * LN2
    inv = 1.0 / total
    for t in range(4):
        out = None
        for m in range(4):
            w = jnp.broadcast_to((ws[m] * inv)[t : t + 1, :], (128, 128)).T
            part = i_ref[m, t * 128 : (t + 1) * 128, :].astype(jnp.float32) * w
            out = part if out is None else out + part
        o_ref[t * 128 : (t + 1) * 128, :] = out


def body(queries, keys, values, positions):
    bf, f32 = jnp.bfloat16, jnp.float32
    core = lax.axis_index("blk") % NC

    packed, qo = call(
        pack_kernel,
        (jax.ShapeDtypeStruct((16, 72, DH), bf), jax.ShapeDtypeStruct((528, DH), bf)),
        "hhhh",
        scratch=[
            SM((512,), jnp.int32),
            VM((32, HK * DH), bf),
            VM((32, HK * DH), bf),
            pltpu.SemaphoreType.DMA((4,)),
        ],
    )(*[pltpu.with_memory_space_constraint(a, pltpu.HBM) for a in (positions, keys, values, queries)])
    got = lax.all_to_all(packed, ("blk", "col"), 0, 0, axis_index_groups=KV_GROUPS, tiled=False)
    qz, qc = send(qo, ZPAIR), send(qo, CORE)
    qd = send(qz, CORE)
    qs = (qo, qz, qc, qd)
    own = call(
        prep_kernel, jax.ShapeDtypeStruct((ROWS, DH), bf), "v", scratch=[VM((BK, DH), f32), SM((NST,), jnp.int32)]
    )(got)

    up, down = [send(own, UP)], [send(own, DOWN)]
    for _ in range(2):
        up.append(send(up[-1], UP))
        down.append(send(down[-1], DOWN))
    far = send(jnp.where(core == 0, up[1], down[1]), LAST)

    acc = jax.ShapeDtypeStruct((NQ, 144, 256), f32)
    top = jax.ShapeDtypeStruct((NQ, 8, 256), f32)

    def attend(blocks, carry, last=False):
        n = len(blocks)
        first = carry is None
        kernel = lambda *refs: attend_kernel(n, first, last, *refs)
        scratch = [
            VM((NQ, 256, DH), bf),
            VM((2, SUB, 256), f32),
            SM((NQ,), jnp.int32),
            SM((NQ,), jnp.int32),
            SM((n * NST,), jnp.int32),
        ]
        if last:
            scratch = [VM(acc.shape, f32), VM(top.shape, f32)] + scratch
        args = qs + tuple(blocks) + (() if first else carry)
        return call(
            kernel,
            jax.ShapeDtypeStruct((4, 528, DH), bf) if last else (acc, top),
            "v" * len(args),
            scratch=scratch,
            alias=None if first or last else {4 + n: 0, 5 + n: 1},
            flops=n * 2_000_000_000,
        )(*args)

    carry = attend([own], None)
    carry = attend([up[0], down[0]], carry)
    carry = attend([up[1], down[1]], carry)
    carry = attend([up[2]], carry)
    part = attend([down[2], far], carry, last=True)
    parts = lax.all_to_all(part, ("blk", "col"), 0, 0, axis_index_groups=OUT_GROUPS, tiled=False)
    attended, lognorm = call(
        merge_kernel, (jax.ShapeDtypeStruct((512, DH), f32), jax.ShapeDtypeStruct((4, 128), f32)), "v"
    )(parts)
    return attended, lognorm.reshape(512, 1)


def solution(mesh):
    placed = (P("blk", "col"), P(("blk", "col"), None), P(("blk", "col"), None), P("blk"))
    return jax.shard_map(
        body,
        mesh=mesh,
        in_specs=placed,
        out_specs=(P("blk", "col"), P("blk", "col")),
        check_vma=False,
    )
```

```python
import math

import jax
import jax.numpy as jnp
from jax import lax
from jax.experimental import pallas as pl
from jax.experimental.pallas import tpu as pltpu
from jax.sharding import PartitionSpec as P


HK = 4
DH = 128
STRIPE = 128
NY, NZH, NC, NX, NZL = 8, 2, 2, 4, 4
SUB = 64
NST = 8
BK = NST * SUB
ROWS = 2 * BK + 16
NQ = 8
C2 = math.log2(math.e) / math.sqrt(DH)
LN2 = math.log(2.0)
MASKED = -1e30
EMPTY = -1e29
VM = pltpu.VMEM
SM = pltpu.SMEM


def flat_groups(key):
    found = {}
    for b in range(NY * NZH * NC):
        for c in range(NX * NZL):
            k = key(b // 4, (b // 2) % 2, b % 2, c // 4, c % 4)
            found.setdefault(k, []).append(b * NX * NZL + c)
    return list(found.values())


KV_GROUPS = flat_groups(lambda y, zh, c, x, zl: (y, c, zl % 2))
OUT_GROUPS = flat_groups(lambda y, zh, c, x, zl: (y, zh, x, zl // 2))


def pairs(move):
    out = []
    for b in range(NY * NZH * NC):
        for c in range(NX * NZL):
            y, zh, co, x, zl = move(b // 4, (b // 2) % 2, b % 2, c // 4, c % 4)
            out.append((b * 16 + c, ((y % NY) * 4 + zh * 2 + co) * 16 + x * 4 + zl))
    return out


UP = pairs(lambda y, zh, c, x, zl: (y + 1, zh, c, x, zl))
DOWN = pairs(lambda y, zh, c, x, zl: (y - 1, zh, c, x, zl))
LAST = pairs(lambda y, zh, c, x, zl: (y + 2 - 4 * c, zh, c, x, zl))
CORE = pairs(lambda y, zh, c, x, zl: (y, zh, 1 - c, x, zl))
ZPAIR = pairs(lambda y, zh, c, x, zl: (y, zh, c, x, zl ^ 1))


def send(value, perm):
    return lax.ppermute(value, ("blk", "col"), perm)


def call(kernel, out, in_spaces, scratch=(), alias=None, flops=0):
    vm = pl.BlockSpec(memory_space=VM)
    sm = pl.BlockSpec(memory_space=SM)
    return pl.pallas_call(
        kernel,
        out_shape=out,
        in_specs=[{"s": sm, "v": vm, "h": pl.BlockSpec(memory_space=pltpu.HBM)}[s] for s in in_spaces],
        out_specs=jax.tree.map(lambda _: vm, out),
        scratch_shapes=list(scratch),
        input_output_aliases=alias or {},
        cost_estimate=pl.CostEstimate(flops=flops, transcendentals=0, bytes_accessed=0) if flops else None,
        compiler_params=pltpu.CompilerParams(vmem_limit_bytes=40 * 1024 * 1024),
    )


def pack_kernel(pos_hbm, k_hbm, v_hbm, q_hbm, o_ref, q_ref, pos, k_ref, v_ref, sems):
    copies = [
        pltpu.make_async_copy(src, dst, sems.at[i])
        for i, (src, dst) in enumerate(
            [(pos_hbm, pos), (k_hbm, k_ref), (v_hbm, v_ref), (q_hbm, q_ref.at[pl.ds(0, 512)])]
        )
    ]
    for c in copies:
        c.start()
    copies[0].wait()
    x = lax.axis_index("col") // NZL
    mine = pos[pl.multiple_of(x * STRIPE, STRIPE)] // STRIPE
    tile = jnp.full((8, DH), mine.astype(jnp.float32), jnp.float32).astype(jnp.bfloat16)
    for m in range(16):
        o_ref[m, 64:72, :] = tile
    row = lax.broadcasted_iota(jnp.int32, (16, DH), 0)
    tile = jnp.zeros((16, DH), jnp.float32)
    for r in range(4):
        tile = jnp.where(row == r, (pos[r * STRIPE] // STRIPE).astype(jnp.float32), tile)
    q_ref[512:528, :] = tile.astype(jnp.bfloat16)
    for at, ref, c in ((0, k_ref, copies[1]), (32, v_ref, copies[2])):
        c.wait()
        for m in range(16):
            head = (m // 2) % 4
            o_ref[m, at : at + 32, :] = ref[:, head * DH : (head + 1) * DH]
    copies[3].wait()


def scalar_of(row):
    return jnp.max(row.astype(jnp.float32)).astype(jnp.int32)


def prep_kernel(r_ref, o_ref, v_scr, p_scr):
    pos = []
    for j in range(NST):
        m = (j // 4) * 8 + (j % 4) * 2
        pos.append(scalar_of(r_ref[m, 64:65, :]))
    for j in range(NST):
        rank = jnp.int32(0)
        for i in range(NST):
            if i != j:
                rank = rank + (pos[i] < pos[j]).astype(jnp.int32)
        p_scr[rank] = pos[j]
        m = (j // 4) * 8 + (j % 4) * 2
        at = pl.multiple_of(rank * SUB, SUB)
        kk = jnp.concatenate([r_ref[m, 0:32, :], r_ref[m + 1, 0:32, :]], axis=0)
        vv = jnp.concatenate([r_ref[m, 32:64, :], r_ref[m + 1, 32:64, :]], axis=0)
        o_ref[pl.ds(at, SUB), :] = kk
        v_scr[pl.ds(at, SUB), :] = vv.astype(jnp.float32)
    for t in range(BK // DH):
        o_ref[BK + t * DH : BK + (t + 1) * DH, :] = v_scr[t * DH : (t + 1) * DH, :].T.astype(jnp.bfloat16)
    row = lax.broadcasted_iota(jnp.int32, (16, DH), 0)
    tile = jnp.zeros((16, DH), jnp.float32)
    for r in range(NST):
        tile = jnp.where(row == r, p_scr[r].astype(jnp.float32), tile)
    o_ref[2 * BK : ROWS, :] = tile.astype(jnp.bfloat16)


def attend_kernel(nblocks, first, last, qo_ref, qz_ref, qc_ref, qd_ref, *rest):
    blocks, rest = rest[:nblocks], list(rest[nblocks:])
    accin_ref, min_ref = (None, None) if first else (rest.pop(0), rest.pop(0))
    out_ref = rest.pop(0) if last else None
    acc_ref, m_ref, q_ref, off_ref, qp, qt, kp = rest
    core = lax.axis_index("blk") % NC
    side = lax.axis_index("col") % 2
    pos = []
    for t in range(4):
        q_ref[t, 0:128, :] = qo_ref[t * 128 : (t + 1) * 128, :]
        q_ref[t, 128:256, :] = qz_ref[t * 128 : (t + 1) * 128, :]
        q_ref[4 + t, 0:128, :] = qc_ref[t * 128 : (t + 1) * 128, :]
        q_ref[4 + t, 128:256, :] = qd_ref[t * 128 : (t + 1) * 128, :]
    for ref in (qo_ref, qc_ref):
        for t in range(4):
            pos.append(scalar_of(ref[512 + t : 513 + t, :]))
    for j in range(NQ):
        rank = jnp.int32(0)
        for i in range(NQ):
            if i != j:
                rank = rank + (pos[i] < pos[j]).astype(jnp.int32)
        qp[rank] = pos[j]
        qt[rank] = jnp.int32(j)
    for n, blk in enumerate(blocks):
        for j in range(NST):
            kp[n * NST + j] = scalar_of(blk[2 * BK + j : 2 * BK + j + 1, :])
    if first:
        r = lax.broadcasted_iota(jnp.int32, (SUB, 256), 0)
        lane = lax.broadcasted_iota(jnp.int32, (SUB, 256), 1)
        off = (r // 32) * 64 + side * 32 + r % 32 - lane % 128
        off_ref[0] = jnp.zeros((SUB, 256), jnp.float32)
        off_ref[1] = jnp.where(off <= 0, 0.0, MASKED)
        acc_ref[...] = jnp.zeros_like(acc_ref)
        m_ref[...] = jnp.full(m_ref.shape, EMPTY, jnp.float32)
    else:
        acc_ref[...] = accin_ref[...]
        m_ref[...] = min_ref[...]
    ones = jnp.ones((16, BK), jnp.bfloat16)

    def scores(t, keys):
        return [
            lax.dot_general(blk[0:keys, :], q_ref[t], (((1,), (1,)), ((), ())), preferred_element_type=jnp.float32)
            for blk in blocks
        ]

    def local(qpos, raw, keys):
        parts = []
        top = None
        for n, s in enumerate(raw):
            runs = []
            for j in range(keys // SUB):
                run = s[j * SUB : (j + 1) * SUB, :]
                kpos = kp[n * NST + j]
                if first:
                    run = run + off_ref[(kpos == qpos).astype(jnp.int32)]
                hidden = jnp.where(kpos <= qpos, 0.0, MASKED).astype(jnp.float32)
                high = jnp.max(run.reshape(SUB // 8, 8, 256), axis=0) * C2 + hidden
                top = high if top is None else jnp.maximum(top, high)
                runs.append((run, hidden))
            parts.append(runs)
        top = jnp.maximum(jnp.max(top, axis=0, keepdims=True), EMPTY)
        mixed = None
        for runs, blk in zip(parts, blocks):
            p = jnp.concatenate([jnp.exp2(run * C2 + (hidden - top)) for run, hidden in runs], axis=0)
            vt = jnp.concatenate(
                [blk[BK + i * DH : BK + (i + 1) * DH, :] for i in range(keys // DH)], axis=1
            )
            vt = jnp.concatenate([vt, ones[:, 0:keys]], axis=0)
            part = jnp.dot(vt, p.astype(jnp.bfloat16), preferred_element_type=jnp.float32)
            mixed = part if mixed is None else mixed + part
        return top, mixed

    size = 2

    def together(i, keys):
        raws = [scores(qt[size * i + k], keys) for k in range(size)]
        found = [(qt[size * i + k],) + local(qp[size * i + k], raws[k], keys) for k in range(size)]
        for t, top, mixed in found:
            old = m_ref[t, 0:1, :]
            new = jnp.maximum(old, top)
            acc_ref[t] = acc_ref[t] * jnp.exp2(old - new) + mixed * jnp.exp2(top - new)
            m_ref[t] = jnp.broadcast_to(new, (8, 256))

    def group(i, carry):
        far = qp[size * i + size - 1]
        need = jnp.int32(0)
        for n in range(nblocks):
            seen = jnp.int32(0)
            for j in (0, 2, 4, 6):
                seen = seen + (kp[n * NST + j] <= far).astype(jnp.int32)
            need = jnp.maximum(need, seen)
        for level, keys in ((1, 2 * SUB), (2, 4 * SUB), (3, 6 * SUB), (4, 8 * SUB)):

            @pl.when(need == level)
            def _(keys=keys):
                together(i, keys)

        return carry

    lax.fori_loop(0, NQ // size, group, 0)
    if last:
        partial(core, side, acc_ref, m_ref, out_ref)


def partial(core, side, acc_ref, m_ref, o_ref):
    for dc in range(2):
        for dz in range(2):
            member = (core + dc - 2 * core * dc) * 2 + (side + dz - 2 * side * dz)
            rows = []
            for t in range(4):
                st = dc * 4 + t
                lanes = slice(dz * 128, dz * 128 + 128)
                total = acc_ref[st, 128:129, lanes]
                top = m_ref[st, 0:1, lanes]
                seen = total > 0.0
                inv = jnp.where(seen, 1.0 / jnp.where(seen, total, 1.0), 0.0)
                o_ref[member, t * 128 : (t + 1) * 128, :] = (acc_ref[st, 0:128, lanes] * inv).T.astype(jnp.bfloat16)
                rows.append(jnp.where(seen, top + jnp.log2(jnp.where(seen, total, 1.0)), EMPTY))
            lse = jnp.concatenate(rows, axis=0)
            hi = lse.astype(jnp.bfloat16).astype(jnp.float32)
            mid = (lse - hi).astype(jnp.bfloat16).astype(jnp.float32)
            low = lse - hi - mid
            o_ref[member, 512:528, :] = jnp.concatenate(
                [hi, mid, low, jnp.zeros((4, 128), jnp.float32)], axis=0
            ).astype(jnp.bfloat16)


def merge_kernel(i_ref, o_ref, l_ref):
    lses = []
    for m in range(4):
        tile = i_ref[m, 512:528, :].astype(jnp.float32)
        lses.append(tile[0:4] + tile[4:8] + tile[8:12])
    top = jnp.maximum(jnp.maximum(lses[0], lses[1]), jnp.maximum(lses[2], lses[3]))
    ws = [jnp.exp2(x - top) for x in lses]
    total = ws[0] + ws[1] + ws[2] + ws[3]
    l_ref[...] = (top + jnp.log2(total)) * LN2
    inv = 1.0 / total
    for t in range(4):
        out = None
        for m in range(4):
            w = jnp.broadcast_to((ws[m] * inv)[t : t + 1, :], (128, 128)).T
            part = i_ref[m, t * 128 : (t + 1) * 128, :].astype(jnp.float32) * w
            out = part if out is None else out + part
        o_ref[t * 128 : (t + 1) * 128, :] = out


def body(queries, keys, values, positions):
    bf, f32 = jnp.bfloat16, jnp.float32
    core = lax.axis_index("blk") % NC

    packed, qo = call(
        pack_kernel,
        (jax.ShapeDtypeStruct((16, 72, DH), bf), jax.ShapeDtypeStruct((528, DH), bf)),
        "hhhh",
        scratch=[
            SM((512,), jnp.int32),
            VM((32, HK * DH), bf),
            VM((32, HK * DH), bf),
            pltpu.SemaphoreType.DMA((4,)),
        ],
    )(*[pltpu.with_memory_space_constraint(a, pltpu.HBM) for a in (positions, keys, values, queries)])
    got = lax.all_to_all(packed, ("blk", "col"), 0, 0, axis_index_groups=KV_GROUPS, tiled=False)
    qz, qc = send(qo, ZPAIR), send(qo, CORE)
    qd = send(qz, CORE)
    qs = (qo, qz, qc, qd)
    own = call(
        prep_kernel, jax.ShapeDtypeStruct((ROWS, DH), bf), "v", scratch=[VM((BK, DH), f32), SM((NST,), jnp.int32)]
    )(got)

    up = [send(own, UP)]
    down = [send(own, DOWN)]
    for _ in range(2):
        up.append(send(up[-1], UP))
        down.append(send(down[-1], DOWN))
    far = send(jnp.where(core == 0, up[1], down[1]), LAST)

    acc = jax.ShapeDtypeStruct((NQ, 144, 256), f32)
    top = jax.ShapeDtypeStruct((NQ, 8, 256), f32)

    def attend(blocks, carry, last=False):
        n = len(blocks)
        first = carry is None
        kernel = lambda *refs: attend_kernel(n, first, last, *refs)
        scratch = [
            VM((NQ, 256, DH), bf),
            VM((2, SUB, 256), f32),
            SM((NQ,), jnp.int32),
            SM((NQ,), jnp.int32),
            SM((n * NST,), jnp.int32),
        ]
        if last:
            scratch = [VM(acc.shape, f32), VM(top.shape, f32)] + scratch
        args = qs + tuple(blocks) + (() if first else carry)
        return call(
            kernel,
            jax.ShapeDtypeStruct((4, 528, DH), bf) if last else (acc, top),
            "v" * len(args),
            scratch=scratch,
            alias=None if first or last else {4 + n: 0, 5 + n: 1},
            flops=n * 2_000_000_000,
        )(*args)

    carry = attend([own], None)
    carry = attend([up[0], down[0]], carry)
    carry = attend([up[1], down[1]], carry)
    carry = attend([up[2], down[2]], carry)
    part = attend([far], carry, last=True)
    parts = lax.all_to_all(part, ("blk", "col"), 0, 0, axis_index_groups=OUT_GROUPS, tiled=False)
    attended, lognorm = call(
        merge_kernel, (jax.ShapeDtypeStruct((512, DH), f32), jax.ShapeDtypeStruct((4, 128), f32)), "v"
    )(parts)
    return attended, lognorm.reshape(512, 1)


def solution(mesh):
    placed = (P("blk", "col"), P(("blk", "col"), None), P(("blk", "col"), None), P("blk"))
    return jax.shard_map(
        body,
        mesh=mesh,
        in_specs=placed,
        out_specs=(P("blk", "col"), P("blk", "col")),
        check_vma=False,
    )
```
